512 devices in a mesh: lat: 16 (over y, z_hi), lon: 4 (over x), fold: 8 (over z_lo, core).
Axes of the slice: x: 4, y: 4, z: 16 (z_hi: 4, z_lo: 4; z = z_hi * 4 + z_lo), core: 2. Of those that a mesh axis runs over, the one named last changes fastest.
Arguments:
- field: float32 [8, 12, 640, 2560], P('fold', None, 'lat', 'lon'), may hold values from -6 to 6
- row_shift: int32 [8, 12, 640, 2560], P('fold', None, 'lat', 'lon'), may hold values from -4 to 4
- col_shift: int32 [8, 12, 640, 2560], P('fold', None, 'lat', 'lon'), may hold values from -4 to 4
- row_frac: bfloat16 [8, 12, 640, 2560], P('fold', None, 'lat', 'lon'), may hold values from 0 to 1
- col_frac: bfloat16 [8, 12, 640, 2560], P('fold', None, 'lat', 'lon'), may hold values from 0 to 1
- wave_map: int32 [64], replicated, may hold values from 0 to 1279, as said below
- legendre: float32 [64, 640, 1280], P('lon', 'lat'), may hold values from -0.25 to 0.25
- helm_coef: float32 [48], P('fold'), may hold values from 1e-06 to 0.0001
Outputs:
- spectrum: float32 [48, 4, 16, 2560], P('fold', 'lon', 'lat')
The draws below stay inside these ranges and needn't reach their ends.
Inputs may be any that keep to these rules, and one draw needn't show every extreme that they name: `col_shift`: longitude offset of the departure cell. `wave_map`: distinct zonal wavenumbers.
All inputs are finite; a program needn't handle non-finite values.
Results may differ from the reference program's by a relative error of at most 0.0003.
Values sent between devices are 32-bit elements; how exact they have to be, the bound alone decides.
A program may use at most 64 MiB of HBM per device.

```python
import math
import jax
import jax.numpy as jnp
from jax import lax

LAT_HALF = 640
LON_CELLS = 2560
DEGREES = 1280
SHIFT_MAX = 4
LEVEL_DEV = 12
GROUPS = 8
LEVELS = 48
WAVES_LON = 16
WAVE_SLOTS = 64
N_LON = 4


def draw_wave_map(key, part):
    ordering = jax.random.permutation(key, DEGREES)
    return ordering[:WAVE_SLOTS].astype(jnp.int32)


def plant(result, key, least, largest):
    shape = result.shape
    index_at = [jax.random.randint(jax.random.fold_in(key, axis), (), 0, shape[axis]) for axis in range(len(shape))]
    result = result.at[tuple(index_at)].set(least)
    longest = shape.index(max(shape))
    index_at[longest] = (index_at[longest] + 1) % shape[longest]
    return result.at[tuple(index_at)].set(largest)


def level_of(key, extent, split, smallest, top_value):
    def one(dim, blocks):
        steps = jax.random.uniform(jax.random.fold_in(jax.random.fold_in(key, 6), dim), (blocks,), jnp.float32, smallest / len(split), top_value / len(split))
        return jnp.repeat(jnp.exp(steps), extent[dim] // blocks).reshape((-1,) + (1,) * (len(extent) - dim - 1))

    level = one(*split[0])
    for cut in split[1:]:
        level = level * one(*cut)
    return level


def gaussian(stream_key, dims, scale, bound, pieces=(), held_as=jnp.bfloat16):
    factor_of = level_of(stream_key, dims, pieces, -0.22, 0.18) if pieces else 1.0
    drawn = jax.random.normal(stream_key, dims, jnp.float32) * scale * factor_of
    return jnp.minimum(jnp.maximum(drawn, -bound), bound).astype(held_as)


def setup_inputs(seed: int = 0) -> dict:
    seeds = jax.random.split(jax.random.key(seed), 9)
    return {
        "field": gaussian(seeds[0], (GROUPS, LEVEL_DEV, LAT_HALF, LON_CELLS), 1.0, 6.0, ((0, 8), (2, 16), (3, 4)), jnp.float32),
        "row_shift": plant(jax.random.randint(seeds[1], (GROUPS, LEVEL_DEV, LAT_HALF, LON_CELLS), 0 - SHIFT_MAX, SHIFT_MAX + 1), jax.random.fold_in(seeds[1], 1), 0 - SHIFT_MAX, SHIFT_MAX).astype(jnp.int32),
        "col_shift": plant(jax.random.randint(seeds[2], (GROUPS, LEVEL_DEV, LAT_HALF, LON_CELLS), 0 - SHIFT_MAX, SHIFT_MAX + 1), jax.random.fold_in(seeds[2], 1), 0 - SHIFT_MAX, SHIFT_MAX).astype(jnp.int32),
        "row_frac": jnp.clip(1.0 * jax.random.uniform(seeds[3], (GROUPS, LEVEL_DEV, LAT_HALF, LON_CELLS), jnp.float32) ** level_of(seeds[3], (GROUPS, LEVEL_DEV, LAT_HALF, LON_CELLS), ((0, 8), (2, 16), (3, 4)), -0.2, 0.2), 0.0, 1.0).astype(jnp.bfloat16),
        "col_frac": jnp.clip(1.0 * jax.random.uniform(seeds[4], (GROUPS, LEVEL_DEV, LAT_HALF, LON_CELLS), jnp.float32) ** level_of(seeds[4], (GROUPS, LEVEL_DEV, LAT_HALF, LON_CELLS), ((0, 8), (2, 16), (3, 4)), -0.2, 0.2), 0.0, 1.0).astype(jnp.bfloat16),
        "wave_map": draw_wave_map(jax.random.fold_in(seeds[8], 71), 0),
        "legendre": gaussian(seeds[6], (WAVE_SLOTS, LAT_HALF, DEGREES), LAT_HALF ** -0.5, 0.25, ((0, 4), (1, 16)), jnp.float32),
        "helm_coef": jnp.clip(jnp.exp(math.log(0.0001) - 4.6051702 * jax.random.uniform(seeds[7], (LEVELS,), jnp.float32) ** level_of(seeds[7], (LEVELS,), ((0, 8),), -0.2, 0.2)), 9.999999974752427e-07, 0.0001),
    }


def cubic_weights(fraction):
    return (-fraction * (fraction - 1.0) * (fraction - 2.0) / 6.0, (fraction + 1.0) * (fraction - 1.0) * (fraction - 2.0) / 2.0, -(fraction + 1.0) * fraction * (fraction - 2.0) / 2.0, (fraction + 1.0) * fraction * (fraction - 1.0) / 6.0)

def interpolate(padded, row_shift, col_shift, row_frac, col_frac, margin):
    levels, rows, cols = row_shift.shape
    width = cols + 2 * margin
    flat = padded.reshape(levels, -1)
    row_base = lax.broadcasted_iota(jnp.int32, (levels, rows, cols), 1) + row_shift + (margin - 1)
    col_base = lax.broadcasted_iota(jnp.int32, (levels, rows, cols), 2) + col_shift + (margin - 1)
    start_index = (row_base * width + col_base).reshape(levels, -1).astype(jnp.int32)
    row_weights = cubic_weights(row_frac.astype(jnp.float32).reshape(levels, -1))
    col_weights = cubic_weights(col_frac.astype(jnp.float32).reshape(levels, -1))
    total = jnp.zeros(start_index.shape, jnp.float32)
    for row_step in range(4):
        line = jnp.zeros(start_index.shape, jnp.float32)
        for col_step in range(4):
            taken = jnp.take_along_axis(flat, start_index + (row_step * width + col_step), axis=1)
            line = line + col_weights[col_step] * taken
        total = total + row_weights[row_step] * line
    return total.reshape(levels, rows, cols)

def zonal_table(waves, first_col, count_cols, lon_total):
    col_ids = first_col + lax.iota(jnp.int32, count_cols)
    phase = col_ids[:, None] * waves[None, :] % lon_total
    angle = phase.astype(jnp.float32) * (2.0 * math.pi / lon_total)
    return jnp.stack([jnp.cos(angle), -jnp.sin(angle)], axis=1) / math.sqrt(lon_total)

def reference(field, row_shift, col_shift, row_frac, col_frac, wave_map, legendre, helm_coef):
    margin = SHIFT_MAX + 2
    blocks = GROUPS // 2
    fields = field.reshape(blocks, 2, LEVEL_DEV, LAT_HALF, LON_CELLS)
    opposite = fields[:, ::-1]
    band = opposite[:, :, :, ::-1, :][:, :, :, :margin, :]
    polar = jnp.zeros((blocks, 2, LEVEL_DEV, margin, LON_CELLS), jnp.float32)
    extended = jnp.concatenate([polar, fields, band], axis=3)
    extended = jnp.concatenate([extended[..., -margin:], extended, extended[..., :margin]], axis=4)
    number = blocks * 2 * LEVEL_DEV

    def one_field(items):
        padded, shift_rows, shift_cols, frac_rows, frac_cols = items
        return interpolate(padded[None], shift_rows[None], shift_cols[None], frac_rows[None], frac_cols[None], margin)[0]
    gridded = lax.map(one_field, (extended.reshape(number, LAT_HALF + 2 * margin, LON_CELLS + 2 * margin), row_shift.reshape(number, LAT_HALF, LON_CELLS), col_shift.reshape(number, LAT_HALF, LON_CELLS), row_frac.reshape(number, LAT_HALF, LON_CELLS), col_frac.reshape(number, LAT_HALF, LON_CELLS)))
    gridded = gridded.reshape(blocks, 2, LEVEL_DEV, LAT_HALF, LON_CELLS)
    even = (gridded[:, 0] + gridded[:, 1]).reshape(LEVELS, LAT_HALF, LON_CELLS)
    odd = (gridded[:, 0] - gridded[:, 1]).reshape(LEVELS, LAT_HALF, LON_CELLS)
    table = zonal_table(wave_map, 0, LON_CELLS, LON_CELLS)
    zonal_even = jnp.einsum('lkx,xqs->lsqk', even, table, precision=lax.Precision.HIGHEST)
    zonal_odd = jnp.einsum('lkx,xqs->lsqk', odd, table, precision=lax.Precision.HIGHEST)
    sum_even = jnp.einsum('lsqk,skn->lsqn', zonal_even, legendre, precision=lax.Precision.HIGHEST)
    sum_odd = jnp.einsum('lsqk,skn->lsqn', zonal_odd, legendre, precision=lax.Precision.HIGHEST)
    degrees = jnp.arange(DEGREES, dtype=jnp.int32)
    parity = (wave_map[:, None] + degrees[None, :]) % 2 == 0
    keep = (degrees[None, :] >= wave_map[:, None]).astype(jnp.float32)
    legendre_sum = jnp.where(parity[None, :, None, :], sum_even, sum_odd) * keep[None, :, None, :]
    degree_float = degrees.astype(jnp.float32)
    damping = 1.0 + helm_coef[:, None, None, None] * (degree_float * (degree_float + 1.0))[None, None, None, :]
    spectrum = legendre_sum / damping
    return spectrum.reshape(LEVELS, N_LON, WAVES_LON, 2 * DEGREES)
```

```python
import functools
import math

import jax
import jax.numpy as jnp
from jax import lax
from jax.experimental import pallas as pl
from jax.experimental.pallas import tpu as pltpu
from jax.sharding import PartitionSpec as P

SHIFT_MAX = 4
LANES = 128
HEAD = 8
HALO = 6
WINDOWS = 6
STEP = 107
EDGE = 5
RING = 4
BATCH = 4
TRIO = 3
VMEM_BYTES = 60000 * 1024


def cubic_weights(t):
    tm, tp, td = t - 1.0, t + 1.0, t - 2.0
    outer = t * tm
    inner = tp * td
    return (
        outer * (td * (-1.0 / 6.0)),
        inner * (tm * 0.5),
        inner * (t * -0.5),
        outer * (tp * (1.0 / 6.0)),
    )


def turned(x, left):
    left = left % LANES
    return pltpu.roll(x, LANES - left, 1) if left else x


def window_start(t):
    return STEP * t - EDGE


def windows_of(tiles, lane):
    out = []
    for t in range(WINDOWS):
        first, left = divmod(window_start(t), LANES)
        a, b = tiles.get(first), tiles.get(first + 1)
        if a is None or b is None:
            out.append(turned(b if a is None else a, left))
        else:
            out.append(jnp.where(lane < LANES - left, turned(a, left), turned(b, left)))
    return out


def angle_parts(phase, lon_total):
    quarter = lon_total // 4
    turn = jnp.floor(phase.astype(jnp.float32) * (1.0 / lon_total)).astype(jnp.int32)
    phase = phase - turn * lon_total
    phase = jnp.where(phase < 0, phase + lon_total, phase)
    phase = jnp.where(phase >= lon_total, phase - lon_total, phase)
    quad = jnp.floor(phase.astype(jnp.float32) * (1.0 / quarter) + 0.5).astype(jnp.int32)
    x = (phase - quad * quarter).astype(jnp.float32) * (2.0 * math.pi / lon_total)
    quad = quad & 3
    y = x * x
    s = x * (1.0 + y * (-1.0 / 6 + y * (1.0 / 120 + y * (-1.0 / 5040 + y * (1.0 / 362880)))))
    c = 1.0 + y * (-0.5 + y * (1.0 / 24 + y * (-1.0 / 720 + y * (1.0 / 40320))))
    swap = (quad & 1) == 1
    cos = jnp.where(swap, s, c)
    sin = jnp.where(swap, c, s)
    cos = jnp.where((quad == 1) | (quad == 2), -cos, cos)
    sin = jnp.where(quad >= 2, -sin, sin)
    return cos, sin


def build_table(waves, table, first_col, cols, lon_total, chunk):
    slots = waves.shape[0]
    scale = 1.0 / math.sqrt(lon_total)
    sub = lax.broadcasted_iota(jnp.int32, (8, LANES), 0)
    lane = lax.broadcasted_iota(jnp.int32, (8, LANES), 1)
    start = first_col + lon_total + jnp.where(lane < WINDOWS, lane * STEP - EDGE, 0)
    rows = 2 * slots
    for v in range(0, slots, 8):
        m = jnp.zeros((8, LANES), jnp.int32)
        for i in range(8):
            m = jnp.where(sub == i, waves[v + i], m)
        cos_lane, sin_lane = angle_parts(m * lane, lon_total)
        cos_start, sin_start = angle_parts(m * start, lon_total)
        at = v // chunk * 2 * chunk + v % chunk
        for t in range(WINDOWS):
            count = min(STEP, cols - STEP * t)
            valid = (lane >= EDGE) & (lane < EDGE + count)
            ca = cos_start[:, t : t + 1] * scale
            sa = sin_start[:, t : t + 1] * scale
            real = jnp.where(valid, ca * cos_lane - sa * sin_lane, 0.0)
            imag = jnp.where(valid, -(sa * cos_lane + ca * sin_lane), 0.0)
            for row, value in ((at, real), (at + chunk, imag)):
                top = value.astype(jnp.bfloat16).astype(jnp.float32)
                table[row : row + 8, t * LANES : (t + 1) * LANES] = top
                table[rows + row : rows + row + 8, t * LANES : (t + 1) * LANES] = value - top


def interpolate_rows(source, steps_r, steps_c, grid, level, start):
    lane = lax.broadcasted_iota(jnp.int32, (8, LANES), 1)
    at = pl.ds(start, 8)

    def spread(ref):
        cols = ref.shape[2]
        return windows_of({t: ref[level, at, t * LANES : (t + 1) * LANES] for t in range(cols // LANES)}, lane)

    place_r, place_c = spread(steps_r), spread(steps_c)
    rows = source.shape[2] - 2 * HEAD
    target = pl.ds(pl.multiple_of(lax.rem(level, TRIO) * rows + start, 8), 8)
    for t in range(WINDOWS):
        base_c = jnp.minimum(jnp.floor(place_c[t]), float(SHIFT_MAX))
        base_r = jnp.minimum(jnp.floor(place_r[t]), float(SHIFT_MAX))
        wc = cubic_weights(place_c[t] - base_c)
        wr = cubic_weights(place_r[t] - base_r)
        first = base_c.astype(jnp.int32) + lane
        index = [(first + (b - 1)) & (LANES - 1) for b in range(4)]
        lines = []
        for offset in range(-SHIFT_MAX - 1, SHIFT_MAX + 3):
            cells = source[level, t, pl.ds(start + (HEAD + offset), 8), :]
            line = None
            for b in range(4):
                taken = jnp.take_along_axis(cells, index[b], axis=1, mode="promise_in_bounds")
                term = wc[b] * taken
                line = term if line is None else line + term
            lines.append(line)
        left = base_r
        far = left >= 1.0
        lines = [jnp.where(far, lines[i + 4], lines[i]) for i in range(8)]
        left = jnp.where(far, left - 4.0, left)
        far = left >= -1.0
        lines = [jnp.where(far, lines[i + 2], lines[i]) for i in range(6)]
        left = jnp.where(far, left - 2.0, left)
        far = left >= -3.0
        lines = [jnp.where(far, lines[i + 1], lines[i]) for i in range(5)]
        left = jnp.where(far, left - 1.0, left)
        far = left >= -3.0
        lines = [jnp.where(far, lines[i + 1], lines[i]) for i in range(4)]
        total = wr[0] * lines[0]
        for a in range(1, 4):
            total = total + wr[a] * lines[a]
        grid[level // TRIO, target, t * LANES : (t + 1) * LANES] = total


def peer_of(fold):
    return fold + 1 - 2 * (fold % 2)


def grid_kernel(
    n_lat,
    n_lon,
    waves,
    field,
    row_shift,
    col_shift,
    row_frac,
    col_frac,
    out,
    packed,
    corner_out,
    landed,
    side,
    corner_in,
    corner_tile,
    steps_r,
    steps_c,
    source,
    grid,
    table,
    row_send,
    row_recv,
    side_send,
    side_recv,
    corner_send,
    corner_recv,
):
    levels, rows, cols = field.shape
    batches = levels // BATCH
    lines = BATCH * HALO
    lat, lon, fold = (lax.axis_index(a) for a in ("lat", "lon", "fold"))
    last = lat == n_lat - 1
    is_last = last.astype(jnp.int32)
    east = lax.rem(lon + 1, n_lon)
    west = lax.rem(lon + n_lon - 1, n_lon)
    below = lat + 1 - is_last
    below_fold = fold + is_last * (1 - 2 * (fold % 2))
    first = lat == 0

    def tail_to(x):
        return {"lat": below, "lon": x, "fold": below_fold}

    def head_to(x):
        return {"lat": lat - 1, "lon": x, "fold": fold}

    barrier = pltpu.get_barrier_semaphore()

    def greet(where):
        pl.semaphore_signal(barrier, inc=1, device_id=where, device_id_type=pl.DeviceIdType.MESH)

    for x in (lon, east, west):
        greet(tail_to(x))
    for x in (east, west):
        greet({"lat": lat, "lon": x, "fold": fold})

    @pl.when(jnp.logical_not(first))
    def _():
        for x in (lon, east, west):
            greet(head_to(x))

    for level in range(levels):
        packed[0, HALO * level : HALO * (level + 1), :] = field[level, 0:HALO, :]

    @pl.when(jnp.logical_not(last))
    def _():
        for level in range(levels):
            packed[1, HALO * level : HALO * (level + 1), :] = field[level, rows - HALO : rows, :]

    @pl.when(last)
    def _():
        for level in range(levels):
            for i in range(HALO):
                at = HALO * level + i
                packed[1, at : at + 1, :] = field[level, rows - 1 - i : rows - i, :]

    lane = lax.broadcasted_iota(jnp.int32, (8, LANES), 1)
    for end in range(2):
        for right in range(2):
            value = jnp.zeros((8, LANES), jnp.float32)
            for g in range(levels * HALO // 8):
                part = packed[end, 8 * g : 8 * g + 8, right * (cols - LANES) : right * (cols - LANES) + LANES]
                part = turned(part, right * (LANES - 8) - 8 * g)
                value = jnp.where((lane >= 8 * g) & (lane < 8 * g + 8), part, value)
            corner_out[end, right] = value

    pl.semaphore_wait(barrier, 8 - 3 * first.astype(jnp.int32))

    def row_copy(end, batch, where, place):
        at = pl.ds(lines * batch, lines)
        return pltpu.make_async_remote_copy(
            src_ref=packed.at[end, at],
            dst_ref=landed.at[place, at],
            send_sem=row_send.at[end, batch],
            recv_sem=row_recv.at[place, batch],
            device_id=where,
            device_id_type=pl.DeviceIdType.MESH,
        )

    def side_copy(right, batch):
        at = pl.ds(BATCH * batch, BATCH)
        return pltpu.make_async_remote_copy(
            src_ref=field.at[at, :, pl.ds(right * (cols - LANES), LANES)],
            dst_ref=side.at[1 - right, at],
            send_sem=side_send.at[right, batch],
            recv_sem=side_recv.at[1 - right, batch],
            device_id={"lat": lat, "lon": east if right else west, "fold": fold},
            device_id_type=pl.DeviceIdType.MESH,
        )

    def corner_copy(end, right, where, place):
        return pltpu.make_async_remote_copy(
            src_ref=corner_out.at[end, right],
            dst_ref=corner_in.at[place, 1 - right],
            send_sem=corner_send.at[end, right],
            recv_sem=corner_recv.at[place, 1 - right],
            device_id=where,
            device_id_type=pl.DeviceIdType.MESH,
        )

    sides = [[side_copy(right, b) for right in range(2)] for b in range(batches)]
    tail_corners = [corner_copy(1, right, tail_to(east if right else west), is_last) for right in range(2)]
    head_corners = [corner_copy(0, right, head_to(east if right else west), 1) for right in range(2)]
    tails = [row_copy(1, b, tail_to(lon), is_last) for b in range(batches)]
    heads = [row_copy(0, b, head_to(lon), 1) for b in range(batches)]
    for copy in tail_corners:
        copy.start()

    @pl.when(jnp.logical_not(first))
    def _():
        for copy in head_corners:
            copy.start()

    for b in range(batches):
        tails[b].start()

        @pl.when(jnp.logical_not(first))
        def _():
            heads[b].start()

        for copy in sides[b]:
            copy.start()

    build_table(waves, table, lon * cols, cols, cols * n_lon, waves.shape[0] // n_lon)
    for trio in range(levels // TRIO):
        grid[trio, TRIO * rows :, :] = jnp.zeros((LANES - TRIO * rows, grid.shape[2]), jnp.float32)

    def prepare(level, carry):
        steps_r[level] = row_shift[level].astype(jnp.float32) + row_frac[level].astype(jnp.float32)
        steps_c[level] = col_shift[level].astype(jnp.float32) + col_frac[level].astype(jnp.float32)
        return carry

    lax.fori_loop(0, levels, prepare, 0)
    count = cols // LANES
    wide = lax.broadcasted_iota(jnp.int32, (rows, LANES), 1)

    def inner(level, carry):
        tiles = {t: field[level, :, t * LANES : (t + 1) * LANES] for t in range(count)}
        tiles[-1] = side[0, level]
        tiles[count] = side[1, level]
        for t, value in enumerate(windows_of(tiles, wide)):
            source[level, t, HEAD : HEAD + rows, :] = value

        def block(j, carry):
            interpolate_rows(source, steps_r, steps_c, grid, level, pl.multiple_of(8 * j, 8))
            return carry

        lax.fori_loop(1, rows // 8 - 1, block, 0)
        return carry

    for b in range(batches):
        for copy in sides[b]:
            copy.wait()
        lax.fori_loop(BATCH * b, BATCH * (b + 1), inner, 0)

    narrow = lax.broadcasted_iota(jnp.int32, (lines, LANES), 1)

    def halo_rows(b):
        at = slice(lines * b, lines * (b + 1))
        for end, to in ((0, HEAD - HALO), (1, HEAD + rows)):
            tiles = {t: landed[end, at, t * LANES : (t + 1) * LANES] for t in range(count)}
            tiles[-1] = corner_tile[end, 0, at, :]
            tiles[count] = corner_tile[end, 1, at, :]
            for t, value in enumerate(windows_of(tiles, narrow)):
                for i in range(BATCH):
                    source[BATCH * b + i, t, to : to + HALO, :] = value[HALO * i : HALO * (i + 1)]

    def outer(level, carry):
        for j in (0, rows // 8 - 1):
            interpolate_rows(source, steps_r, steps_c, grid, level, 8 * j)
        return carry

    def spread_corners(end):
        for right in range(2):
            value = corner_in[end, right]
            for g in range(levels * HALO // 8):
                corner_tile[end, right, 8 * g : 8 * g + 8, :] = turned(value, 8 * g - (0 if right else LANES - 8))

    for copy in tail_corners:
        copy.wait_send()

    @pl.when(jnp.logical_not(first))
    def _():
        for right in range(2):
            head_corners[right].wait_send()
            corner_copy(0, 1 - right, head_to(lon), 0).wait_recv()
        spread_corners(0)

    @pl.when(first)
    def _():
        landed[0] = jnp.zeros(landed.shape[1:], jnp.float32)
        corner_tile[0] = jnp.zeros(corner_tile.shape[1:], jnp.float32)

    for right in range(2):
        corner_copy(0, 1 - right, head_to(lon), 1).wait_recv()
    spread_corners(1)

    full = table.shape[0] // 2
    done = 0
    for b in range(batches):
        tails[b].wait_send()
        row_copy(0, b, head_to(lon), 1).wait_recv()

        @pl.when(jnp.logical_not(first))
        def _():
            heads[b].wait_send()
            row_copy(0, b, head_to(lon), 0).wait_recv()

        halo_rows(b)
        lax.fori_loop(BATCH * b, BATCH * (b + 1), outer, 0)
        ready = BATCH * (b + 1) // TRIO
        for trio in range(done, ready):
            values = grid[trio]
            top = values.astype(jnp.bfloat16)
            rest = (values - top.astype(jnp.float32)).astype(jnp.bfloat16)
            factors = table[...].astype(jnp.bfloat16)
            dims = (((1,), (1,)), ((), ()))
            both = lax.dot_general(factors, top, dims, preferred_element_type=jnp.float32)
            more = lax.dot_general(factors[:full], rest, dims, preferred_element_type=jnp.float32)
            out[trio] = both[:full] + both[full:] + more
        done = ready


def grid_waves(wave_map, field, shifts, fracs):
    levels, rows, cols = field.shape
    n_lat, n_lon = lax.axis_size("lat"), lax.axis_size("lon")
    vmem = pl.BlockSpec(memory_space=pltpu.VMEM)
    batches = levels // BATCH
    halo_rows = levels * HALO
    f32 = jnp.float32
    full = 2 * wave_map.shape[0]
    dma = pltpu.SemaphoreType.DMA
    return pl.pallas_call(
        functools.partial(grid_kernel, n_lat, n_lon),
        in_specs=[pl.BlockSpec(memory_space=pltpu.SMEM)] + [vmem] * 5,
        out_specs=vmem,
        out_shape=jax.ShapeDtypeStruct((levels // TRIO, full, LANES), f32),
        scratch_shapes=[
            pltpu.VMEM((2, halo_rows, cols), f32),
            pltpu.VMEM((2, 2, 8, LANES), f32),
            pltpu.VMEM((2, halo_rows, cols), f32),
            pltpu.VMEM((2, levels, rows, LANES), f32),
            pltpu.VMEM((2, 2, 8, LANES), f32),
            pltpu.VMEM((2, 2, halo_rows, LANES), f32),
            pltpu.VMEM((levels, rows, cols), f32),
            pltpu.VMEM((levels, rows, cols), f32),
            pltpu.VMEM((levels, WINDOWS, rows + 2 * HEAD, LANES), f32),
            pltpu.VMEM((levels // TRIO, LANES, WINDOWS * LANES), f32),
            pltpu.VMEM((2 * full, WINDOWS * LANES), f32),
            dma((2, batches)),
            dma((2, batches)),
            dma((2, batches)),
            dma((2, batches)),
            dma((2, 2)),
            dma((2, 2)),
        ],
        compiler_params=pltpu.CompilerParams(
            collective_id=0, has_side_effects=True, vmem_limit_bytes=VMEM_BYTES
        ),
        name="grid_waves",
    )(wave_map, field, *shifts, *fracs)


def spectral_kernel(
    n_lon,
    waves,
    helm,
    zonal,
    legendre,
    out,
    landed,
    total,
    mirrored,
    left_side,
    right_side,
    piece,
    y_far,
    y_left,
    y_right,
    joined,
    z_far,
    z_left,
    z_right,
    lon_send,
    lon_recv,
    fold_send,
    fold_recv,
    y_send,
    y_recv,
    z_send,
    z_recv,
):
    trios, full, _ = zonal.shape
    slots, rows, degrees = legendre.shape
    half = degrees // 2
    per = out.shape[0]
    lat, lon, fold = (lax.axis_index(a) for a in ("lat", "lon", "fold"))
    hemisphere = fold % 2
    mine = trios // 2
    y, z = lat // RING, lat % RING
    chunk = full // n_lon

    def at_ring(dy, dz):
        return {
            "lat": lax.rem(y + dy + RING, RING) * RING + lax.rem(z + dz + RING, RING),
            "lon": lon,
            "fold": fold,
        }

    def at_lon(dx):
        return {"lat": lat, "lon": lax.rem(lon + dx, n_lon), "fold": fold}

    partner = {"lat": lat, "lon": lon, "fold": peer_of(fold)}
    barrier = pltpu.get_barrier_semaphore()
    friends = [at_lon(dx) for dx in range(1, n_lon)] + [partner]
    friends += [at_ring(1, 0), at_ring(-1, 0), at_ring(0, 1), at_ring(0, -1)]
    for where in friends:
        pl.semaphore_signal(barrier, inc=1, device_id=where, device_id_type=pl.DeviceIdType.MESH)
    pl.semaphore_wait(barrier, len(friends))

    def remote(src, dst, send, recv, where):
        return pltpu.make_async_remote_copy(
            src_ref=src,
            dst_ref=dst,
            send_sem=send,
            recv_sem=recv,
            device_id=where,
            device_id_type=pl.DeviceIdType.MESH,
        )

    def chunk_of(x):
        return pl.ds(pl.multiple_of(x * chunk, chunk), chunk)

    lon_copies = []
    for dx in range(1, n_lon):
        copy = remote(
            zonal.at[:, chunk_of(lax.rem(lon + dx, n_lon))],
            landed.at[dx - 1],
            lon_send.at[dx - 1],
            lon_recv.at[dx - 1],
            at_lon(dx),
        )
        copy.start()
        lon_copies.append(copy)

    def split(s, carry):
        for a in range(0, degrees, 2 * LANES):
            cut = slice(a, a + 2 * LANES)
            value = legendre[s, :, cut]
            top = value.astype(jnp.bfloat16).astype(jnp.float32)
            rest = value - top
            fill = jnp.zeros((LANES - 3 * rows, 2 * LANES), jnp.float32)
            right_side[s, :, cut] = jnp.concatenate([top, top, rest, fill], axis=0).astype(jnp.bfloat16)
        return carry

    lax.fori_loop(0, slots, split, 0)
    left_side[...] = jnp.zeros(left_side.shape, jnp.float32)

    for copy in lon_copies:
        copy.wait()
    total[...] = zonal[:, chunk_of(lon), :] + landed[0] + landed[1] + landed[2]
    fold_copy = remote(
        total.at[pl.ds((1 - hemisphere) * mine, mine)], mirrored, fold_send.at[0], fold_recv.at[0], partner
    )
    fold_copy.start()
    fold_copy.wait()
    sign = (1 - 2 * hemisphere).astype(jnp.float32)
    kept = total[pl.ds(hemisphere * mine, mine)]
    other = mirrored[...]
    pair = (kept + other, sign * (kept - other))
    lane = lax.broadcasted_iota(jnp.int32, (slots, LANES), 1)
    for parity in range(2):
        for q in range(mine):
            for part in range(2):
                block = pair[parity][q, part * slots : (part + 1) * slots]
                for i in range(TRIO):
                    value = jnp.where(lane < rows, turned(block, i * rows), 0.0)
                    top = value.astype(jnp.bfloat16).astype(jnp.float32)
                    rest = value - top
                    value = top + turned(rest, -rows) + turned(top, -2 * rows)
                    row = parity * 16 + part * per + q * TRIO + i
                    left_side[pl.ds(row, slots, 32), :] = value

    count = 2 * per
    column = lax.broadcasted_iota(jnp.int32, (1, half), 1)
    offsets = (2, 1, 3, 0)
    cuts = ((pl.ds(0, 384), pl.ds(384, 256)), (pl.ds(384, 256), pl.ds(0, 384)))
    up, down = at_ring(1, 0), at_ring(-1, 0)
    above, under = at_ring(0, 1), at_ring(0, -1)

    def compute(k, dy):
        slot = lax.rem(y + dy, RING) * RING + lax.rem(z + offsets[k], RING)
        wave = waves[lon * slots + slot]
        left = left_side[pl.ds(pl.multiple_of(slot * 32, 32), 32), :].astype(jnp.bfloat16)
        for h in range(2):
            product = jnp.dot(left, right_side[slot, :, h * half : (h + 1) * half], preferred_element_type=jnp.float32)
            degree = column + h * half
            even = ((wave + degree) & 1) == 0
            value = jnp.where(even, product[:16], product[16:])
            value = jnp.where(degree >= wave, value, 0.0)
            piece[k, dy, h * count : (h + 1) * count, :] = value[:count]

    first_pairs, last_pairs = [], []
    plain = []
    for k in range(RING):
        big, small = cuts[k % 2]

        def y_copy(i, src, dst, where):
            return remote(src, dst, y_send.at[k, i], y_recv.at[k, i], where)

        compute(k, 2)
        one = y_copy(0, piece.at[k, 2, :, big], y_far.at[k, :, big], up)
        two = y_copy(1, piece.at[k, 2, :, small], y_far.at[k, :, small], down)
        one.start()
        two.start()
        compute(k, 1)
        three = y_copy(2, piece.at[k, 1, :, small], y_left.at[k, :, small], up)
        three.start()
        compute(k, 3)
        four = y_copy(3, piece.at[k, 3, :, big], y_right.at[k, :, big], down)
        four.start()
        compute(k, 0)
        five = y_copy(4, piece.at[k, 1, :, big], y_left.at[k, :, big], up)
        six = y_copy(5, piece.at[k, 3, :, small], y_right.at[k, :, small], down)
        first_pairs.append((one, two))
        plain.append((three, four))
        last_pairs.append((five, six))

    def forward(k):
        big, small = cuts[k % 2]
        one, two = first_pairs[k]
        five, six = last_pairs[k]
        one.wait_recv()
        piece[k, 1, :, big] = piece[k, 1, :, big] + y_far[k, :, big]
        five.start()
        two.wait_recv()
        piece[k, 3, :, small] = piece[k, 3, :, small] + y_far[k, :, small]
        six.start()

    def settle(k):
        for copy in plain[k] + last_pairs[k]:
            copy.wait_recv()
        joined[k] = piece[k, 0] + y_left[k] + y_right[k]

    big, small = cuts[0]

    def z_copy(i, src, dst, where):
        return remote(src, dst, z_send.at[i], z_recv.at[i], where)

    z_copies = [
        z_copy(0, joined.at[0, :, big], z_far.at[:, big], above),
        z_copy(1, joined.at[0, :, small], z_far.at[:, small], under),
        z_copy(2, joined.at[1, :, small], z_left.at[:, small], above),
        z_copy(3, joined.at[2, :, big], z_right.at[:, big], under),
        z_copy(4, joined.at[1, :, big], z_left.at[:, big], above),
        z_copy(5, joined.at[2, :, small], z_right.at[:, small], under),
    ]
    forward(0)
    forward(1)
    settle(0)
    z_copies[0].start()
    z_copies[1].start()
    forward(2)
    settle(1)
    z_copies[2].start()
    forward(3)
    settle(2)
    z_copies[3].start()
    z_copies[0].wait_recv()
    joined[1, :, big] = joined[1, :, big] + z_far[:, big]
    z_copies[4].start()
    z_copies[1].wait_recv()
    joined[2, :, small] = joined[2, :, small] + z_far[:, small]
    z_copies[5].start()
    settle(3)
    row = lax.broadcasted_iota(jnp.int32, (2 * count, half), 0)
    degree = lax.broadcasted_iota(jnp.int32, (2 * count, half), 1) + jnp.where(row >= count, half, 0)
    degree = degree.astype(jnp.float32)
    factor = jnp.zeros((2 * count, half), jnp.float32)
    for r in range(2 * count):
        factor = jnp.where(row == r, helm[r % per], factor)
    damping = 1.0 + factor * (degree * (degree + 1.0))
    for copy in z_copies[2:]:
        copy.wait_recv()
    result = (joined[3] + z_left[...] + z_right[...]) / damping
    for r in range(2 * count):
        h, part, level = r // count, r % count // per, r % per
        at = part * degrees + h * half
        out[level, 0, :, at : at + half] = result[r : r + 1]
    for copies in first_pairs + plain + last_pairs:
        for copy in copies:
            copy.wait_send()
    for copy in z_copies:
        copy.wait_send()


def spectrum_of(wave_map, helm, zonal, legendre):
    n_lon = lax.axis_size("lon")
    trios, full, _ = zonal.shape
    slots, rows, degrees = legendre.shape
    per = helm.shape[0]
    vmem = pl.BlockSpec(memory_space=pltpu.VMEM)
    smem = pl.BlockSpec(memory_space=pltpu.SMEM)
    f32 = jnp.float32
    block = (4 * per, degrees // 2)
    dma = pltpu.SemaphoreType.DMA
    return pl.pallas_call(
        functools.partial(spectral_kernel, n_lon),
        in_specs=[smem, smem, vmem, vmem],
        out_specs=vmem,
        out_shape=jax.ShapeDtypeStruct((per, 1, 1, 2 * degrees), f32),
        scratch_shapes=[
            pltpu.VMEM((n_lon - 1, trios, full // n_lon, LANES), f32),
            pltpu.VMEM((trios, full // n_lon, LANES), f32),
            pltpu.VMEM((trios // 2, full // n_lon, LANES), f32),
            pltpu.VMEM((slots * 32, LANES), f32),
            pltpu.VMEM((slots, LANES, degrees), jnp.bfloat16),
            pltpu.VMEM((RING, RING) + block, f32),
            pltpu.VMEM((RING,) + block, f32),
            pltpu.VMEM((RING,) + block, f32),
            pltpu.VMEM((RING,) + block, f32),
            pltpu.VMEM((RING,) + block, f32),
            pltpu.VMEM(block, f32),
            pltpu.VMEM(block, f32),
            pltpu.VMEM(block, f32),
            dma((n_lon - 1,)),
            dma((n_lon - 1,)),
            dma((1,)),
            dma((1,)),
            dma((RING, 6)),
            dma((RING, 6)),
            dma((6,)),
            dma((6,)),
        ],
        compiler_params=pltpu.CompilerParams(
            collective_id=1, has_side_effects=True, vmem_limit_bytes=VMEM_BYTES
        ),
        name="spectrum",
    )(wave_map, helm, zonal, legendre)


def local(field, row_shift, col_shift, row_frac, col_frac, wave_map, legendre, helm_coef):
    zonal = grid_waves(wave_map, field[0], (row_shift[0], col_shift[0]), (row_frac[0], col_frac[0]))
    return spectrum_of(wave_map, helm_coef, zonal, legendre)


def solution(mesh):
    block = P("fold", None, "lat", "lon")
    in_specs = (block,) * 5 + (P(), P("lon", "lat", None), P("fold"))
    out_specs = P("fold", "lon", "lat", None)
    return jax.shard_map(local, mesh=mesh, in_specs=in_specs, out_specs=out_specs, check_vma=False)
```

```python
import functools
import math

import jax
import jax.numpy as jnp
from jax import lax
from jax.experimental import pallas as pl
from jax.experimental.pallas import tpu as pltpu
from jax.sharding import PartitionSpec as P

SHIFT_MAX = 4
LANES = 128
HEAD = 8
HALO = 6
RING = 4
BATCHES = 3
PAIR = 2
VMEM_BYTES = 60000 * 1024


def cubic_weights(t):
    tm, tp, td = t - 1.0, t + 1.0, t - 2.0
    outer = t * tm
    inner = tp * td
    return (
        outer * (td * (-1.0 / 6.0)),
        inner * (tm * 0.5),
        inner * (t * -0.5),
        outer * (tp * (1.0 / 6.0)),
    )


def turned(x, left):
    left = left % LANES
    return pltpu.roll(x, LANES - left, 1) if left else x


def angle_parts(phase, lon_total):
    quarter = lon_total // 4
    turn = jnp.floor(phase.astype(jnp.float32) * (1.0 / lon_total)).astype(jnp.int32)
    phase = phase - turn * lon_total
    phase = jnp.where(phase < 0, phase + lon_total, phase)
    phase = jnp.where(phase >= lon_total, phase - lon_total, phase)
    quad = jnp.floor(phase.astype(jnp.float32) * (1.0 / quarter) + 0.5).astype(jnp.int32)
    x = (phase - quad * quarter).astype(jnp.float32) * (2.0 * math.pi / lon_total)
    quad = quad & 3
    y = x * x
    s = x * (1.0 + y * (-1.0 / 6 + y * (1.0 / 120 + y * (-1.0 / 5040 + y * (1.0 / 362880)))))
    c = 1.0 + y * (-0.5 + y * (1.0 / 24 + y * (-1.0 / 720 + y * (1.0 / 40320))))
    swap = (quad & 1) == 1
    cos = jnp.where(swap, s, c)
    sin = jnp.where(swap, c, s)
    cos = jnp.where((quad == 1) | (quad == 2), -cos, cos)
    sin = jnp.where(quad >= 2, -sin, sin)
    return cos, sin


def build_table(waves, table, first_col, cols, lon_total, chunk):
    slots = waves.shape[0]
    scale = 1.0 / math.sqrt(lon_total)
    sub = lax.broadcasted_iota(jnp.int32, (8, LANES), 0)
    lane = lax.broadcasted_iota(jnp.int32, (8, LANES), 1)
    count = cols // LANES
    start = first_col + jnp.where(lane < count, lane * LANES, 0)
    rows = 2 * slots
    for v in range(0, slots, 8):
        m = jnp.zeros((8, LANES), jnp.int32)
        for i in range(8):
            m = jnp.where(sub == i, waves[v + i], m)
        cos_lane, sin_lane = angle_parts(m * lane, lon_total)
        cos_start, sin_start = angle_parts(m * start, lon_total)
        at = v // chunk * 2 * chunk + v % chunk
        for t in range(count):
            ca = cos_start[:, t : t + 1] * scale
            sa = sin_start[:, t : t + 1] * scale
            real = ca * cos_lane - sa * sin_lane
            imag = -(sa * cos_lane + ca * sin_lane)
            for row, value in ((at, real), (at + chunk, imag)):
                top = value.astype(jnp.bfloat16).astype(jnp.float32)
                table[row : row + 8, t * LANES : (t + 1) * LANES] = top
                table[rows + row : rows + row + 8, t * LANES : (t + 1) * LANES] = value - top


def shifted(tiles, count, lane):
    for c in range(2 * HALO):
        move = c + 1 - HALO
        side = (move > 0) - (move < 0)
        near = {t: turned(tiles[t], move) for t in range(min(0, side), count + max(0, side))}
        for t in range(count):
            if side > 0:
                value = jnp.where(lane < LANES - move, near[t], near[t + 1])
            elif side < 0:
                value = jnp.where(lane >= -move, near[t], near[t - 1])
            else:
                value = near[t]
            yield c, t, value


def interpolate_tile(source, pair, t, start, col_shift, row_shift, col_t, row_t):
    wc = cubic_weights(col_t)
    wr = cubic_weights(row_t)
    size = 2 * HALO
    hits = [col_shift == v for v in range(-SHIFT_MAX, SHIFT_MAX + 1)]
    spread = []
    for place in range(size):
        w = None
        for step in range(4):
            v = place - step
            if 0 <= v < len(hits):
                w = jnp.where(hits[v], wc[step], 0.0 if w is None else w)
        spread.append(w)
    lines = []
    for slot in range(size):
        at = pl.ds(start + (HEAD + 1 - HALO + slot), 8)
        line = None
        for c in range(size):
            term = spread[c] * source[pair, c, t, at, :]
            line = term if line is None else line + term
        lines.append(line)
    left = row_shift
    for reach, least in ((4, 1), (2, -1), (1, -3)):
        far = left >= least
        lines = [jnp.where(far, lines[i + reach], lines[i]) for i in range(len(lines) - reach)]
        left = jnp.where(far, left - reach, left)
    far = left >= -3
    lines = [jnp.where(far, lines[i + 1], lines[i]) for i in range(4)]
    total = wr[0] * lines[0]
    for a in range(1, 4):
        total = total + wr[a] * lines[a]
    return total


def fused_kernel(
    n_lat,
    n_lon,
    waves,
    helm,
    field,
    row_shift_far,
    col_shift_far,
    row_frac_far,
    col_frac_far,
    legendre_far,
    out,
    row_shift,
    col_shift,
    row_frac,
    col_frac,
    legendre,
    packed,
    corner_out,
    side_out,
    landed,
    side,
    side_in,
    corner_in,
    corner_tile,
    row_t,
    col_t,
    source_even,
    source_odd,
    grid,
    table,
    zonal,
    lon_in,
    total,
    mirrored,
    left_side,
    right_side,
    piece,
    y_far,
    y_left,
    y_right,
    joined,
    z_far,
    z_left,
    z_right,
    load_sem,
    row_send,
    row_recv,
    side_send,
    side_recv,
    corner_send,
    corner_recv,
    lon_send,
    lon_recv,
    fold_send,
    fold_recv,
    y_send,
    y_recv,
    z_send,
    z_recv,
):
    levels, rows, cols = field.shape
    half_levels = levels // 2
    slots, _, degrees = legendre.shape
    half = degrees // 2
    count = cols // LANES
    blocks = rows // 8
    lines = 2 * PAIR * HALO
    full = 2 * waves.shape[0]
    chunk = full // n_lon
    sources = (source_even, source_odd)
    lat, lon, fold = (lax.axis_index(a) for a in ("lat", "lon", "fold"))
    hemisphere = fold % 2
    last = lat == n_lat - 1
    is_last = last.astype(jnp.int32)
    east = lax.rem(lon + 1, n_lon)
    west = lax.rem(lon + n_lon - 1, n_lon)
    below = lat + 1 - is_last
    across = fold + 1 - 2 * hemisphere
    below_fold = fold + is_last * (1 - 2 * hemisphere)
    first = lat == 0
    inner_lat = jnp.logical_not(first)
    y, z = lat // RING, lat % RING

    loads = [
        pltpu.make_async_copy(far, near, load_sem.at[i])
        for i, (far, near) in enumerate(
            (
                (row_shift_far, row_shift),
                (col_shift_far, col_shift),
                (row_frac_far, row_frac),
                (col_frac_far, col_frac),
                (legendre_far, legendre),
            )
        )
    ]
    for copy in loads:
        copy.start()

    def tail_to(x):
        return {"lat": below, "lon": x, "fold": below_fold}

    def head_to(x):
        return {"lat": lat - 1, "lon": x, "fold": fold}

    def at_ring(dy, dz):
        return {
            "lat": lax.rem(y + dy + RING, RING) * RING + lax.rem(z + dz + RING, RING),
            "lon": lon,
            "fold": fold,
        }

    def at_lon(dx):
        return {"lat": lat, "lon": lax.rem(lon + dx, n_lon), "fold": fold}

    partner = {"lat": lat, "lon": lon, "fold": across}
    up, down = at_ring(1, 0), at_ring(-1, 0)
    above, under = at_ring(0, 1), at_ring(0, -1)
    barrier = pltpu.get_barrier_semaphore()

    def greet(where):
        pl.semaphore_signal(barrier, inc=1, device_id=where, device_id_type=pl.DeviceIdType.MESH)

    friends = [tail_to(x) for x in (lon, east, west)]
    friends += [at_lon(dx) for dx in range(1, n_lon)] + [partner, up, down, above, under]
    for where in friends:
        greet(where)

    @pl.when(inner_lat)
    def _():
        for x in (lon, east, west):
            greet(head_to(x))

    def remote(src, dst, send, recv, where):
        return pltpu.make_async_remote_copy(
            src_ref=src,
            dst_ref=dst,
            send_sem=send,
            recv_sem=recv,
            device_id=where,
            device_id_type=pl.DeviceIdType.MESH,
        )

    def packed_row(level):
        part, rest = divmod(level, half_levels)
        return lines * (rest // PAIR) + HALO * (PAIR * part + rest % PAIR)

    for level in range(levels):
        packed[0, packed_row(level) : packed_row(level) + HALO, :] = field[level, 0:HALO, :]

    @pl.when(jnp.logical_not(last))
    def _():
        for level in range(levels):
            packed[1, packed_row(level) : packed_row(level) + HALO, :] = field[level, rows - HALO : rows, :]

    @pl.when(last)
    def _():
        for level in range(levels):
            for i in range(HALO):
                at = packed_row(level) + i
                packed[1, at : at + 1, :] = field[level, rows - 1 - i : rows - i, :]

    lane = lax.broadcasted_iota(jnp.int32, (8, LANES), 1)
    for end in range(2):
        for right in range(2):
            value = jnp.zeros((8, LANES), jnp.float32)
            for g in range(levels * HALO // 8):
                part = packed[end, 8 * g : 8 * g + 8, right * (cols - LANES) : right * (cols - LANES) + LANES]
                part = turned(part, right * (LANES - 8) - 8 * g)
                value = jnp.where((lane >= 8 * g) & (lane < 8 * g + 8), part, value)
            corner_out[end, right] = value

    places = LANES // 8
    for right in range(2):
        for v in range(side_out.shape[1]):
            value = jnp.zeros((8, LANES), jnp.float32)
            for i in range(places):
                level, j = divmod(places * v + i, blocks)
                if level < levels:
                    part = field[level, 8 * j : 8 * j + 8, right * (cols - LANES) : right * (cols - LANES) + LANES]
                    part = turned(part, right * (LANES - 8) - 8 * i)
                    value = jnp.where((lane >= 8 * i) & (lane < 8 * i + 8), part, value)
            side_out[right, v] = value

    pl.semaphore_wait(barrier, len(friends) + 3 - 3 * first.astype(jnp.int32))

    def row_copy(end, batch, where, place):
        at = pl.ds(lines * batch, lines)
        return remote(
            packed.at[end, at], landed.at[place, at], row_send.at[end, batch], row_recv.at[place, batch], where
        )

    def corner_copy(end, right, where, place):
        return remote(
            corner_out.at[end, right],
            corner_in.at[place, 1 - right],
            corner_send.at[end, right],
            corner_recv.at[place, 1 - right],
            where,
        )

    sides = [
        remote(
            side_out.at[right],
            side_in.at[1 - right],
            side_send.at[right],
            side_recv.at[1 - right],
            {"lat": lat, "lon": east if right else west, "fold": fold},
        )
        for right in range(2)
    ]
    tail_corners = [corner_copy(1, right, tail_to(east if right else west), is_last) for right in range(2)]
    head_corners = [corner_copy(0, right, head_to(east if right else west), 1) for right in range(2)]
    tails = [row_copy(1, b, tail_to(lon), is_last) for b in range(BATCHES)]
    heads = [row_copy(0, b, head_to(lon), 1) for b in range(BATCHES)]
    for copy in sides + tail_corners:
        copy.start()

    @pl.when(inner_lat)
    def _():
        for copy in head_corners:
            copy.start()

    for b in range(BATCHES):
        tails[b].start()

        @pl.when(inner_lat)
        def _():
            heads[b].start()

    build_table(waves, table, lon * cols, cols, cols * n_lon, waves.shape[0] // n_lon)
    for b in range(BATCHES):
        for h in range(2):
            spare = slice(h * LANES + PAIR * rows, (h + 1) * LANES)
            grid[b, spare, :] = jnp.zeros((LANES - PAIR * rows, cols), jnp.float32)
    left_side[...] = jnp.zeros(left_side.shape, jnp.float32)
    for copy in loads:
        copy.wait()

    def prepare(level, carry):
        row_t[level] = row_frac[level].astype(jnp.float32)
        col_t[level] = col_frac[level].astype(jnp.float32)
        return carry

    lax.fori_loop(0, levels, prepare, 0)

    def split(s, carry):
        for a in range(0, degrees, 2 * LANES):
            cut = slice(a, a + 2 * LANES)
            value = legendre[s, :, cut]
            top = value.astype(jnp.bfloat16).astype(jnp.float32)
            rest = value - top
            fill = jnp.zeros((LANES - 3 * rows, 2 * LANES), jnp.float32)
            right_side[s, :, cut] = jnp.concatenate([top, top, rest, fill], axis=0).astype(jnp.bfloat16)
        return carry

    lax.fori_loop(0, slots, split, 0)

    for copy in sides:
        copy.wait()
    for right in range(2):
        for v in range(side_in.shape[1]):
            value = side_in[right, v]
            for i in range(places):
                level, j = divmod(places * v + i, blocks)
                if level < levels:
                    side[right, level, 8 * j : 8 * j + 8, :] = turned(value, 8 * i - (0 if right else LANES - 8))

    def build(target, pair, level, start, size):
        at = pl.ds(start, size)
        to = pl.ds(pl.multiple_of(start + HEAD, 8), size)
        tiles = {t: field[level, at, t * LANES : (t + 1) * LANES] for t in range(count)}
        tiles[-1] = side[0, level, at, :]
        tiles[count] = side[1, level, at, :]
        for c, t, value in shifted(tiles, count, lax.broadcasted_iota(jnp.int32, (size, LANES), 1)):
            target[pair, c, t, to, :] = value

    def interpolate(source, pair, level, start):
        part = level // half_levels
        batch = level % half_levels // PAIR
        to = pl.ds(pl.multiple_of(part * LANES + level % PAIR * rows + start, 8), 8)
        at = pl.ds(start, 8)
        for t in range(count):
            cut = slice(t * LANES, (t + 1) * LANES)
            grid[batch, to, cut] = interpolate_tile(
                source,
                pair,
                t,
                start,
                col_shift[level, at, cut],
                row_shift[level, at, cut],
                col_t[level, at, cut],
                row_t[level, at, cut],
            )

    build(source_even, 0, 0, 0, rows)

    def inner(pair, carry):
        for parity in range(2):
            level = 2 * pair + parity
            if parity == 0:
                ahead, ahead_pair = level + 1, pair
            else:
                ahead_pair = jnp.minimum(pair + 1, half_levels - 1)
                ahead = 2 * ahead_pair

            def step(j, carry):
                interpolate(sources[parity], pair, level, pl.multiple_of(8 * (j + 1), 8))
                start = pl.multiple_of(jnp.minimum(16 * j, rows - 16), 8)
                build(sources[1 - parity], ahead_pair, ahead, start, 16)
                return carry

            lax.fori_loop(0, blocks - 2, step, 0)
        return carry

    lax.fori_loop(0, half_levels, inner, 0)

    def spread_corners(end):
        for right in range(2):
            value = corner_in[end, right]
            for g in range(levels * HALO // 8):
                corner_tile[end, right, 8 * g : 8 * g + 8, :] = turned(value, 8 * g - (0 if right else LANES - 8))

    for copy in tail_corners:
        copy.wait_send()

    @pl.when(inner_lat)
    def _():
        for right in range(2):
            head_corners[right].wait_send()
            corner_copy(0, 1 - right, head_to(lon), 0).wait_recv()
        spread_corners(0)

    @pl.when(first)
    def _():
        landed[0] = jnp.zeros(landed.shape[1:], jnp.float32)
        corner_tile[0] = jnp.zeros(corner_tile.shape[1:], jnp.float32)

    for right in range(2):
        corner_copy(0, 1 - right, head_to(lon), 1).wait_recv()
    spread_corners(1)

    narrow = lax.broadcasted_iota(jnp.int32, (lines, LANES), 1)

    def edges(b):
        tails[b].wait_send()
        row_copy(0, b, head_to(lon), 1).wait_recv()

        @pl.when(inner_lat)
        def _():
            heads[b].wait_send()
            row_copy(0, b, head_to(lon), 0).wait_recv()

        at = slice(lines * b, lines * (b + 1))
        for end, to in ((0, HEAD - HALO), (1, HEAD + rows)):
            tiles = {t: landed[end, at, t * LANES : (t + 1) * LANES] for t in range(count)}
            tiles[-1] = corner_tile[end, 0, at, :]
            tiles[count] = corner_tile[end, 1, at, :]
            for c, t, value in shifted(tiles, count, narrow):
                for q in range(2 * PAIR):
                    pair = q // PAIR * (half_levels // 2) + b
                    sources[q % 2][pair, c, t, to : to + HALO, :] = value[HALO * q : HALO * (q + 1)]

        def both(h, carry):
            pair = h * (half_levels // 2) + b

            def end(e, carry):
                for parity in range(2):
                    start = pl.multiple_of(e * (rows - 8), 8)
                    interpolate(sources[parity], pair, 2 * pair + parity, start)
                return carry

            return lax.fori_loop(0, 2, end, carry)

        lax.fori_loop(0, 2, both, 0)

    def chunk_of(x):
        return pl.ds(pl.multiple_of(x * chunk, chunk), chunk)

    lon_copies = [
        [
            remote(
                zonal.at[b, chunk_of(lax.rem(lon + dx, n_lon))],
                lon_in.at[b, dx - 1],
                lon_send.at[b, dx - 1],
                lon_recv.at[b, dx - 1],
                at_lon(dx),
            )
            for dx in range(1, n_lon)
        ]
        for b in range(BATCHES)
    ]
    fold_copies = [
        remote(total.at[b, 1 - hemisphere], mirrored.at[b], fold_send.at[b], fold_recv.at[b], partner)
        for b in range(BATCHES)
    ]

    def transform(b):
        values = grid[b]
        top = values.astype(jnp.bfloat16)
        rest = (values - top.astype(jnp.float32)).astype(jnp.bfloat16)
        factors = table[...].astype(jnp.bfloat16)
        dims = (((1,), (1,)), ((), ()))
        wide = lax.dot_general(factors, top, dims, preferred_element_type=jnp.float32)
        more = lax.dot_general(factors[:full], rest, dims, preferred_element_type=jnp.float32)
        zonal[b] = wide[:full] + wide[full:] + more
        for copy in lon_copies[b]:
            copy.start()

    def gather_lon(b):
        for copy in lon_copies[b]:
            copy.wait_recv()
        value = zonal[b, chunk_of(lon), :]
        for dx in range(1, n_lon):
            value = value + lon_in[b, dx - 1]
        for h in range(2):
            total[b, h] = value[:, h * LANES : (h + 1) * LANES]
        fold_copies[b].start()

    column = lax.broadcasted_iota(jnp.int32, (1, degrees), 1)
    row = lax.broadcasted_iota(jnp.int32, (8, half), 0)
    slot_lane = lax.broadcasted_iota(jnp.int32, (slots, LANES), 1)
    big, small = pl.ds(0, 384), pl.ds(384, 256)
    big_of = [(big, small), (small, big), (big, small)]

    y_copies, z_copies = [], []
    for b in range(BATCHES):
        one, two = big_of[b]

        def y_copy(i, src, dst, where):
            return remote(src, dst, y_send.at[b, i], y_recv.at[b, i], where)

        def z_copy(i, src, dst, where):
            return remote(src, dst, z_send.at[b, i], z_recv.at[b, i], where)

        y_copies.append(
            [
                y_copy(0, piece.at[b, 2, :, :, one], y_far.at[b, :, :, one], up),
                y_copy(1, piece.at[b, 2, :, :, two], y_far.at[b, :, :, two], down),
                y_copy(2, piece.at[b, 1, :, :, two], y_left.at[b, :, :, two], up),
                y_copy(3, piece.at[b, 3, :, :, one], y_right.at[b, :, :, one], down),
                y_copy(4, piece.at[b, 1, :, :, one], y_left.at[b, :, :, one], up),
                y_copy(5, piece.at[b, 3, :, :, two], y_right.at[b, :, :, two], down),
            ]
        )
        z_copies.append(
            [
                z_copy(0, joined.at[b, 2, :, one], z_far.at[b, :, one], above),
                z_copy(1, joined.at[b, 2, :, two], z_far.at[b, :, two], under),
                z_copy(2, joined.at[b, 1, :, two], z_left.at[b, :, two], above),
                z_copy(3, joined.at[b, 3, :, one], z_right.at[b, :, one], under),
                z_copy(4, joined.at[b, 1, :, one], z_left.at[b, :, one], above),
                z_copy(5, joined.at[b, 3, :, two], z_right.at[b, :, two], under),
            ]
        )

    def associate(b):
        fold_copies[b].wait_recv()
        sign = (1 - 2 * hemisphere).astype(jnp.float32)
        kept = total[b, hemisphere]
        other = mirrored[b]
        for parity, value in enumerate((kept + other, sign * (kept - other))):
            for part in range(2):
                block = value[part * slots : (part + 1) * slots]
                for i in range(PAIR):
                    cell = jnp.where(slot_lane < rows, turned(block, i * rows), 0.0)
                    top = cell.astype(jnp.bfloat16).astype(jnp.float32)
                    cell = top + turned(cell - top, -rows) + turned(top, -2 * rows)
                    left_side[pl.ds(parity * 8 + part * PAIR + i, slots, 16), :] = cell
        for dy in (2, 1, 3, 0):

            def one(dz, carry):
                slot = lax.rem(y + dy, RING) * RING + lax.rem(z + dz, RING)
                wave = waves[lon * slots + slot]
                left = left_side[pl.ds(pl.multiple_of(slot * 16, 16), 16), :].astype(jnp.bfloat16)
                product = jnp.dot(left, right_side[slot], preferred_element_type=jnp.float32)
                even = ((wave + column) & 1) == 0
                value = jnp.where(even, product[:8], product[8:])
                value = jnp.where(column >= wave, value, 0.0)
                piece[b, dy, dz] = jnp.where(row < 4, value[:, :half], pltpu.roll(value[:, half:], 4, 0))
                return carry

            for dz in range(RING):
                one(dz, 0)
            starts = {2: (0, 1), 1: (2,), 3: (3,), 0: ()}[dy]
            for i in starts:
                y_copies[b][i].start()

    def y_forward(b):
        one, two = big_of[b]
        y_copies[b][0].wait_recv()
        piece[b, 1, :, :, one] = piece[b, 1, :, :, one] + y_far[b, :, :, one]
        y_copies[b][4].start()
        y_copies[b][1].wait_recv()
        piece[b, 3, :, :, two] = piece[b, 3, :, :, two] + y_far[b, :, :, two]
        y_copies[b][5].start()

    def y_settle(b):
        for i in range(2, 6):
            y_copies[b][i].wait_recv()
        joined[b] = piece[b, 0] + y_left[b] + y_right[b]
        for i in range(4):
            z_copies[b][i].start()

    def z_forward(b):
        one, two = big_of[b]
        z_copies[b][0].wait_recv()
        joined[b, 1, :, one] = joined[b, 1, :, one] + z_far[b, :, one]
        z_copies[b][4].start()
        z_copies[b][1].wait_recv()
        joined[b, 3, :, two] = joined[b, 3, :, two] + z_far[b, :, two]
        z_copies[b][5].start()

    degree = lax.broadcasted_iota(jnp.int32, (8, half), 1) + jnp.where(row >= 4, half, 0)
    degree = degree.astype(jnp.float32)
    degree = degree * (degree + 1.0)

    def z_settle(b):
        damping = jnp.where(row % PAIR == 0, helm[PAIR * b], helm[PAIR * b + 1]) * degree + 1.0
        for i in range(2, 6):
            z_copies[b][i].wait_recv()
        result = (joined[b, 0] + z_left[b] + z_right[b]) / damping
        for r in range(8):
            h, part, i = r // 4, r // 2 % 2, r % 2
            at = part * degrees + h * half
            out[PAIR * b + i, 0, :, at : at + half] = result[r : r + 1]

    edges(0)
    transform(0)
    edges(1)
    transform(1)
    gather_lon(0)
    gather_lon(1)
    associate(0)
    edges(2)
    transform(2)
    y_forward(0)
    associate(1)
    gather_lon(2)
    y_settle(0)
    y_forward(1)
    associate(2)
    y_settle(1)
    z_forward(0)
    y_forward(2)
    z_forward(1)
    z_settle(0)
    y_settle(2)
    z_settle(1)
    z_forward(2)
    z_settle(2)
    for b in range(BATCHES):
        for copy in lon_copies[b] + [fold_copies[b]] + y_copies[b] + z_copies[b]:
            copy.wait_send()


def spectrum_of(wave_map, helm, field, shifts, fracs, legendre):
    levels, rows, cols = field.shape
    n_lat, n_lon = lax.axis_size("lat"), lax.axis_size("lon")
    slots, _, degrees = legendre.shape
    vmem = pl.BlockSpec(memory_space=pltpu.VMEM)
    smem = pl.BlockSpec(memory_space=pltpu.SMEM)
    anywhere = pl.BlockSpec(memory_space=pl.ANY)
    halo_rows = levels * HALO
    side_tiles = pl.cdiv(levels * rows, LANES)
    f32 = jnp.float32
    full = 2 * wave_map.shape[0]
    chunk = full // n_lon
    count = cols // LANES
    block = (8, degrees // 2)
    dma = pltpu.SemaphoreType.DMA
    source = pltpu.VMEM((levels // 2, 2 * HALO, count, rows + 2 * HEAD, LANES), f32)
    return pl.pallas_call(
        functools.partial(fused_kernel, n_lat, n_lon),
        in_specs=[smem, smem, vmem] + [anywhere] * 5,
        out_specs=vmem,
        out_shape=jax.ShapeDtypeStruct((levels // 2, 1, 1, 2 * degrees), f32),
        scratch_shapes=[
            pltpu.VMEM((levels, rows, cols), jnp.int32),
            pltpu.VMEM((levels, rows, cols), jnp.int32),
            pltpu.VMEM((levels, rows, cols), jnp.bfloat16),
            pltpu.VMEM((levels, rows, cols), jnp.bfloat16),
            pltpu.VMEM((slots, rows, degrees), f32),
            pltpu.VMEM((2, halo_rows, cols), f32),
            pltpu.VMEM((2, 2, 8, LANES), f32),
            pltpu.VMEM((2, side_tiles, 8, LANES), f32),
            pltpu.VMEM((2, halo_rows, cols), f32),
            pltpu.VMEM((2, levels, rows, LANES), f32),
            pltpu.VMEM((2, side_tiles, 8, LANES), f32),
            pltpu.VMEM((2, 2, 8, LANES), f32),
            pltpu.VMEM((2, 2, halo_rows, LANES), f32),
            pltpu.VMEM((levels, rows, cols), f32),
            pltpu.VMEM((levels, rows, cols), f32),
            source,
            source,
            pltpu.VMEM((BATCHES, 2 * LANES, cols), f32),
            pltpu.VMEM((2 * full, cols), f32),
            pltpu.VMEM((BATCHES, full, 2 * LANES), f32),
            pltpu.VMEM((BATCHES, n_lon - 1, chunk, 2 * LANES), f32),
            pltpu.VMEM((BATCHES, 2, chunk, LANES), f32),
            pltpu.VMEM((BATCHES, chunk, LANES), f32),
            pltpu.VMEM((slots * 16, LANES), f32),
            pltpu.VMEM((slots, LANES, degrees), jnp.bfloat16),
            pltpu.VMEM((BATCHES, RING, RING) + block, f32),
            pltpu.VMEM((BATCHES, RING) + block, f32),
            pltpu.VMEM((BATCHES, RING) + block, f32),
            pltpu.VMEM((BATCHES, RING) + block, f32),
            pltpu.VMEM((BATCHES, RING) + block, f32),
            pltpu.VMEM((BATCHES,) + block, f32),
            pltpu.VMEM((BATCHES,) + block, f32),
            pltpu.VMEM((BATCHES,) + block, f32),
            dma((5,)),
            dma((2, BATCHES)),
            dma((2, BATCHES)),
            dma((2,)),
            dma((2,)),
            dma((2, 2)),
            dma((2, 2)),
            dma((BATCHES, n_lon - 1)),
            dma((BATCHES, n_lon - 1)),
            dma((BATCHES,)),
            dma((BATCHES,)),
            dma((BATCHES, 6)),
            dma((BATCHES, 6)),
            dma((BATCHES, 6)),
            dma((BATCHES, 6)),
        ],
        compiler_params=pltpu.CompilerParams(
            collective_id=0, has_side_effects=True, vmem_limit_bytes=VMEM_BYTES
        ),
        name="spectrum",
    )(wave_map, helm, field, *shifts, *fracs, legendre)


def local(field, row_shift, col_shift, row_frac, col_frac, wave_map, legendre, helm_coef):
    return spectrum_of(
        wave_map,
        helm_coef,
        field[0],
        (row_shift[0], col_shift[0]),
        (row_frac[0], col_frac[0]),
        legendre,
    )


def solution(mesh):
    block = P("fold", None, "lat", "lon")
    in_specs = (block,) * 5 + (P(), P("lon", "lat", None), P("fold"))
    out_specs = P("fold", "lon", "lat", None)
    return jax.shard_map(local, mesh=mesh, in_specs=in_specs, out_specs=out_specs, check_vma=False)
```

```python
import functools
import math

import jax
import jax.numpy as jnp
from jax import lax
from jax.experimental import pallas as pl
from jax.experimental.pallas import tpu as pltpu
from jax.sharding import PartitionSpec as P

SHIFT_MAX = 4
LANES = 128
HEAD = 8
HALO = 6
RING = 4
BATCHES = 3
PAIR = 2
VMEM_BYTES = 60000 * 1024


def cubic_weights(t):
    tm, tp, td = t - 1.0, t + 1.0, t - 2.0
    outer = t * tm
    inner = tp * td
    return (
        outer * (td * (-1.0 / 6.0)),
        inner * (tm * 0.5),
        inner * (t * -0.5),
        outer * (tp * (1.0 / 6.0)),
    )


def turned(x, left):
    left = left % LANES
    return pltpu.roll(x, LANES - left, 1) if left else x


def angle_parts(phase, lon_total):
    quarter = lon_total // 4
    turn = jnp.floor(phase.astype(jnp.float32) * (1.0 / lon_total)).astype(jnp.int32)
    phase = phase - turn * lon_total
    phase = jnp.where(phase < 0, phase + lon_total, phase)
    phase = jnp.where(phase >= lon_total, phase - lon_total, phase)
    quad = jnp.floor(phase.astype(jnp.float32) * (1.0 / quarter) + 0.5).astype(jnp.int32)
    x = (phase - quad * quarter).astype(jnp.float32) * (2.0 * math.pi / lon_total)
    quad = quad & 3
    y = x * x
    s = x * (1.0 + y * (-1.0 / 6 + y * (1.0 / 120 + y * (-1.0 / 5040 + y * (1.0 / 362880)))))
    c = 1.0 + y * (-0.5 + y * (1.0 / 24 + y * (-1.0 / 720 + y * (1.0 / 40320))))
    swap = (quad & 1) == 1
    cos = jnp.where(swap, s, c)
    sin = jnp.where(swap, c, s)
    cos = jnp.where((quad == 1) | (quad == 2), -cos, cos)
    sin = jnp.where(quad >= 2, -sin, sin)
    return cos, sin


def build_table(waves, table, first_col, cols, lon_total, chunk):
    slots = waves.shape[0]
    scale = 1.0 / math.sqrt(lon_total)
    sub = lax.broadcasted_iota(jnp.int32, (8, LANES), 0)
    lane = lax.broadcasted_iota(jnp.int32, (8, LANES), 1)
    count = cols // LANES
    start = first_col + jnp.where(lane < count, lane * LANES, 0)
    rows = 2 * slots
    for v in range(0, slots, 8):
        m = jnp.zeros((8, LANES), jnp.int32)
        for i in range(8):
            m = jnp.where(sub == i, waves[v + i], m)
        cos_lane, sin_lane = angle_parts(m * lane, lon_total)
        cos_start, sin_start = angle_parts(m * start, lon_total)
        at = v // chunk * 2 * chunk + v % chunk
        for t in range(count):
            ca = cos_start[:, t : t + 1] * scale
            sa = sin_start[:, t : t + 1] * scale
            real = ca * cos_lane - sa * sin_lane
            imag = -(sa * cos_lane + ca * sin_lane)
            for row, value in ((at, real), (at + chunk, imag)):
                top = value.astype(jnp.bfloat16).astype(jnp.float32)
                table[row : row + 8, t * LANES : (t + 1) * LANES] = top
                table[rows + row : rows + row + 8, t * LANES : (t + 1) * LANES] = value - top


def shifted(tiles, count, lane):
    for c in range(2 * HALO):
        move = c + 1 - HALO
        side = (move > 0) - (move < 0)
        near = {t: turned(tiles[t], move) for t in range(min(0, side), count + max(0, side))}
        for t in range(count):
            if side > 0:
                value = jnp.where(lane < LANES - move, near[t], near[t + 1])
            elif side < 0:
                value = jnp.where(lane >= -move, near[t], near[t - 1])
            else:
                value = near[t]
            yield c, t, value


def interpolate_tile(source, pair, t, start, col_shift, row_shift, col_t, row_t):
    wc = cubic_weights(col_t)
    wr = cubic_weights(row_t)
    size = 2 * HALO
    hits = [col_shift == v for v in range(-SHIFT_MAX, SHIFT_MAX + 1)]
    spread = []
    for place in range(size):
        w = None
        for step in range(4):
            v = place - step
            if 0 <= v < len(hits):
                w = jnp.where(hits[v], wc[step], 0.0 if w is None else w)
        spread.append(w)
    lines = []
    for slot in range(size):
        at = pl.ds(start + (HEAD + 1 - HALO + slot), 8)
        line = None
        for c in range(size):
            term = spread[c] * source[pair, c, t, at, :]
            line = term if line is None else line + term
        lines.append(line)
    left = row_shift
    for reach, least in ((4, 1), (2, -1), (1, -3)):
        far = left >= least
        lines = [jnp.where(far, lines[i + reach], lines[i]) for i in range(len(lines) - reach)]
        left = jnp.where(far, left - reach, left)
    far = left >= -3
    lines = [jnp.where(far, lines[i + 1], lines[i]) for i in range(4)]
    total = wr[0] * lines[0]
    for a in range(1, 4):
        total = total + wr[a] * lines[a]
    return total


def fused_kernel(
    n_lat,
    n_lon,
    waves,
    helm,
    field,
    row_shift_far,
    col_shift_far,
    row_frac_far,
    col_frac_far,
    legendre_far,
    out,
    row_shift,
    col_shift,
    row_frac,
    col_frac,
    legendre,
    packed,
    corner_out,
    side_out,
    landed,
    side,
    side_in,
    corner_in,
    corner_tile,
    row_t,
    col_t,
    source_even,
    source_odd,
    grid,
    table,
    zonal,
    lon_in,
    left_side,
    right_side,
    piece,
    y_far,
    y_left,
    y_right,
    joined,
    z_far,
    z_left,
    z_right,
    load_sem,
    row_send,
    row_recv,
    side_send,
    side_recv,
    corner_send,
    corner_recv,
    lon_send,
    lon_recv,
    y_send,
    y_recv,
    z_send,
    z_recv,
):
    levels, rows, cols = field.shape
    half_levels = levels // 2
    slots, _, degrees = legendre.shape
    half = degrees // 2
    count = cols // LANES
    blocks = rows // 8
    lines = 2 * PAIR * HALO
    full = 2 * waves.shape[0]
    chunk = full // n_lon
    sources = (source_even, source_odd)
    lat, lon, fold = (lax.axis_index(a) for a in ("lat", "lon", "fold"))
    hemisphere = fold % 2
    last = lat == n_lat - 1
    is_last = last.astype(jnp.int32)
    east = lax.rem(lon + 1, n_lon)
    west = lax.rem(lon + n_lon - 1, n_lon)
    below = lat + 1 - is_last
    across = fold + 1 - 2 * hemisphere
    below_fold = fold + is_last * (1 - 2 * hemisphere)
    first = lat == 0
    inner_lat = jnp.logical_not(first)
    y, z = lat // RING, lat % RING

    loads = [
        pltpu.make_async_copy(far, near, load_sem.at[i])
        for i, (far, near) in enumerate(
            (
                (row_shift_far, row_shift),
                (col_shift_far, col_shift),
                (row_frac_far, row_frac),
                (col_frac_far, col_frac),
                (legendre_far, legendre),
            )
        )
    ]
    for copy in loads:
        copy.start()

    def tail_to(x):
        return {"lat": below, "lon": x, "fold": below_fold}

    def head_to(x):
        return {"lat": lat - 1, "lon": x, "fold": fold}

    def at_ring(dy, dz):
        return {
            "lat": lax.rem(y + dy + RING, RING) * RING + lax.rem(z + dz + RING, RING),
            "lon": lon,
            "fold": fold,
        }

    def at_lon(dx, o):
        return {"lat": lat, "lon": lax.rem(lon + dx, n_lon), "fold": across if o else fold}

    up, down = at_ring(1, 0), at_ring(-1, 0)
    above, under = at_ring(0, 1), at_ring(0, -1)
    barrier = pltpu.get_barrier_semaphore()

    def greet(where):
        pl.semaphore_signal(barrier, inc=1, device_id=where, device_id_type=pl.DeviceIdType.MESH)

    friends = [tail_to(x) for x in (lon, east, west)]
    friends += [at_lon(dx, o) for o in range(2) for dx in range(n_lon) if o or dx] + [up, down, above, under]
    for where in friends:
        greet(where)

    @pl.when(inner_lat)
    def _():
        for x in (lon, east, west):
            greet(head_to(x))

    def remote(src, dst, send, recv, where):
        return pltpu.make_async_remote_copy(
            src_ref=src,
            dst_ref=dst,
            send_sem=send,
            recv_sem=recv,
            device_id=where,
            device_id_type=pl.DeviceIdType.MESH,
        )

    def packed_row(level):
        part, rest = divmod(level, half_levels)
        return lines * (rest // PAIR) + HALO * (PAIR * part + rest % PAIR)

    for level in range(levels):
        packed[0, packed_row(level) : packed_row(level) + HALO, :] = field[level, 0:HALO, :]

    @pl.when(jnp.logical_not(last))
    def _():
        for level in range(levels):
            packed[1, packed_row(level) : packed_row(level) + HALO, :] = field[level, rows - HALO : rows, :]

    @pl.when(last)
    def _():
        for level in range(levels):
            for i in range(HALO):
                at = packed_row(level) + i
                packed[1, at : at + 1, :] = field[level, rows - 1 - i : rows - i, :]

    lane = lax.broadcasted_iota(jnp.int32, (8, LANES), 1)
    for end in range(2):
        for right in range(2):
            value = jnp.zeros((8, LANES), jnp.float32)
            for g in range(levels * HALO // 8):
                part = packed[end, 8 * g : 8 * g + 8, right * (cols - LANES) : right * (cols - LANES) + LANES]
                part = turned(part, right * (LANES - 8) - 8 * g)
                value = jnp.where((lane >= 8 * g) & (lane < 8 * g + 8), part, value)
            corner_out[end, right] = value

    places = LANES // 8
    for right in range(2):
        for v in range(side_out.shape[1]):
            value = jnp.zeros((8, LANES), jnp.float32)
            for i in range(places):
                level, j = divmod(places * v + i, blocks)
                if level < levels:
                    part = field[level, 8 * j : 8 * j + 8, right * (cols - LANES) : right * (cols - LANES) + LANES]
                    part = turned(part, right * (LANES - 8) - 8 * i)
                    value = jnp.where((lane >= 8 * i) & (lane < 8 * i + 8), part, value)
            side_out[right, v] = value

    pl.semaphore_wait(barrier, len(friends) + 3 - 3 * first.astype(jnp.int32))

    def row_copy(end, batch, where, place):
        at = pl.ds(lines * batch, lines)
        return remote(
            packed.at[end, at], landed.at[place, at], row_send.at[end, batch], row_recv.at[place, batch], where
        )

    def corner_copy(end, right, where, place):
        return remote(
            corner_out.at[end, right],
            corner_in.at[place, 1 - right],
            corner_send.at[end, right],
            corner_recv.at[place, 1 - right],
            where,
        )

    sides = [
        remote(
            side_out.at[right],
            side_in.at[1 - right],
            side_send.at[right],
            side_recv.at[1 - right],
            {"lat": lat, "lon": east if right else west, "fold": fold},
        )
        for right in range(2)
    ]
    tail_corners = [corner_copy(1, right, tail_to(east if right else west), is_last) for right in range(2)]
    head_corners = [corner_copy(0, right, head_to(east if right else west), 1) for right in range(2)]
    tails = [row_copy(1, b, tail_to(lon), is_last) for b in range(BATCHES)]
    heads = [row_copy(0, b, head_to(lon), 1) for b in range(BATCHES)]
    for copy in sides + tail_corners:
        copy.start()

    @pl.when(inner_lat)
    def _():
        for copy in head_corners:
            copy.start()

    def send_rows(b):
        if b:
            tails[b - 1].wait_send()
        tails[b].start()

        @pl.when(inner_lat)
        def _():
            if b:
                heads[b - 1].wait_send()
            heads[b].start()

    send_rows(0)
    build_table(waves, table, lon * cols, cols, cols * n_lon, waves.shape[0] // n_lon)
    for b in range(BATCHES):
        for h in range(2):
            spare = slice(h * LANES + PAIR * rows, (h + 1) * LANES)
            grid[b, spare, :] = jnp.zeros((LANES - PAIR * rows, cols), jnp.float32)
    left_side[...] = jnp.zeros(left_side.shape, jnp.float32)
    for copy in loads:
        copy.wait()

    def prepare(level, carry):
        row_t[level] = row_frac[level].astype(jnp.float32)
        col_t[level] = col_frac[level].astype(jnp.float32)
        return carry

    lax.fori_loop(0, levels, prepare, 0)

    def split(s, carry):
        for a in range(0, degrees, 2 * LANES):
            cut = slice(a, a + 2 * LANES)
            value = legendre[s, :, cut]
            top = value.astype(jnp.bfloat16).astype(jnp.float32)
            rest = value - top
            fill = jnp.zeros((LANES - 3 * rows, 2 * LANES), jnp.float32)
            right_side[s, :, cut] = jnp.concatenate([top, top, rest, fill], axis=0).astype(jnp.bfloat16)
        return carry

    lax.fori_loop(0, slots, split, 0)

    for copy in sides:
        copy.wait()
    for right in range(2):
        for v in range(side_in.shape[1]):
            value = side_in[right, v]
            for i in range(places):
                level, j = divmod(places * v + i, blocks)
                if level < levels:
                    side[right, level, 8 * j : 8 * j + 8, :] = turned(value, 8 * i - (0 if right else LANES - 8))

    def build(target, pair, level, start, size):
        at = pl.ds(start, size)
        to = pl.ds(pl.multiple_of(start + HEAD, 8), size)
        tiles = {t: field[level, at, t * LANES : (t + 1) * LANES] for t in range(count)}
        tiles[-1] = side[0, level, at, :]
        tiles[count] = side[1, level, at, :]
        for c, t, value in shifted(tiles, count, lax.broadcasted_iota(jnp.int32, (size, LANES), 1)):
            target[pair, c, t, to, :] = value

    def interpolate(source, pair, level, start):
        part = level // half_levels
        batch = level % half_levels // PAIR
        to = pl.ds(pl.multiple_of(part * LANES + level % PAIR * rows + start, 8), 8)
        at = pl.ds(start, 8)
        for t in range(count):
            cut = slice(t * LANES, (t + 1) * LANES)
            grid[batch, to, cut] = interpolate_tile(
                source,
                pair,
                t,
                start,
                col_shift[level, at, cut],
                row_shift[level, at, cut],
                col_t[level, at, cut],
                row_t[level, at, cut],
            )

    build(source_even, 0, 0, 0, rows)

    def pair_at(n):
        return n // 2 + half_levels // 2 * (n % 2)

    def inner(n, carry):
        pair = pair_at(n)
        for parity in range(2):
            level = 2 * pair + parity
            if parity == 0:
                ahead, ahead_pair = level + 1, pair
            else:
                ahead_pair = pair_at(jnp.minimum(n + 1, half_levels - 1))
                ahead = 2 * ahead_pair

            def step(j, carry):
                interpolate(sources[parity], pair, level, pl.multiple_of(8 * (j + 1), 8))
                start = pl.multiple_of(jnp.minimum(16 * j, rows - 16), 8)
                build(sources[1 - parity], ahead_pair, ahead, start, 16)
                return carry

            lax.fori_loop(0, blocks - 2, step, 0)
        return carry

    def interior(b):
        lax.fori_loop(2 * b, 2 * b + 2, inner, 0)

    def spread_corners(end):
        for right in range(2):
            value = corner_in[end, right]
            for g in range(levels * HALO // 8):
                corner_tile[end, right, 8 * g : 8 * g + 8, :] = turned(value, 8 * g - (0 if right else LANES - 8))

    def corners():
        for copy in tail_corners:
            copy.wait_send()

        @pl.when(inner_lat)
        def _():
            for right in range(2):
                head_corners[right].wait_send()
                corner_copy(0, 1 - right, head_to(lon), 0).wait_recv()
            spread_corners(0)

        @pl.when(first)
        def _():
            landed[0] = jnp.zeros(landed.shape[1:], jnp.float32)
            corner_tile[0] = jnp.zeros(corner_tile.shape[1:], jnp.float32)

        for right in range(2):
            corner_copy(0, 1 - right, head_to(lon), 1).wait_recv()
        spread_corners(1)

    narrow = lax.broadcasted_iota(jnp.int32, (lines, LANES), 1)

    def edges(b):
        if b == BATCHES - 1:
            tails[b].wait_send()
        row_copy(0, b, head_to(lon), 1).wait_recv()

        @pl.when(inner_lat)
        def _():
            if b == BATCHES - 1:
                heads[b].wait_send()
            row_copy(0, b, head_to(lon), 0).wait_recv()

        at = slice(lines * b, lines * (b + 1))
        for end, to in ((0, HEAD - HALO), (1, HEAD + rows)):
            tiles = {t: landed[end, at, t * LANES : (t + 1) * LANES] for t in range(count)}
            tiles[-1] = corner_tile[end, 0, at, :]
            tiles[count] = corner_tile[end, 1, at, :]
            for c, t, value in shifted(tiles, count, narrow):
                for q in range(2 * PAIR):
                    pair = q // PAIR * (half_levels // 2) + b
                    sources[q % 2][pair, c, t, to : to + HALO, :] = value[HALO * q : HALO * (q + 1)]

        def both(h, carry):
            pair = h * (half_levels // 2) + b

            def end(e, carry):
                for parity in range(2):
                    start = pl.multiple_of(e * (rows - 8), 8)
                    interpolate(sources[parity], pair, 2 * pair + parity, start)
                return carry

            return lax.fori_loop(0, 2, end, carry)

        lax.fori_loop(0, 2, both, 0)

    def chunk_of(x):
        return pl.ds(pl.multiple_of(x * chunk, chunk), chunk)

    ways = [(o, dx) for o in range(2) for dx in range(n_lon) if o or dx]
    lon_copies = [
        [
            remote(
                zonal.at[b, 1 - hemisphere if o else hemisphere, chunk_of(lax.rem(lon + dx, n_lon))],
                lon_in.at[b, o, dx],
                lon_send.at[b, o, dx],
                lon_recv.at[b, o, dx],
                at_lon(dx, o),
            )
            for o, dx in ways
        ]
        for b in range(BATCHES)
    ]

    def transform(b):
        values = grid[b]
        top = values.astype(jnp.bfloat16)
        rest = (values - top.astype(jnp.float32)).astype(jnp.bfloat16)
        factors = table[...].astype(jnp.bfloat16)
        dims = (((1,), (1,)), ((), ()))
        wide = lax.dot_general(factors, top, dims, preferred_element_type=jnp.float32)
        more = lax.dot_general(factors[:full], rest, dims, preferred_element_type=jnp.float32)
        value = wide[:full] + wide[full:] + more
        for h in range(2):
            zonal[b, h] = value[:, h * LANES : (h + 1) * LANES]
        for copy in lon_copies[b]:
            copy.start()

    column = lax.broadcasted_iota(jnp.int32, (1, degrees), 1)
    row = lax.broadcasted_iota(jnp.int32, (8, half), 0)
    slot_lane = lax.broadcasted_iota(jnp.int32, (slots, LANES), 1)
    big, small = pl.ds(0, 384), pl.ds(384, 256)
    big_of = [(big, small), (small, big), (big, small)]

    y_copies, z_copies = [], []
    for b in range(BATCHES):
        one, two = big_of[b]

        def y_copy(i, src, dst, where):
            return remote(src, dst, y_send.at[b, i], y_recv.at[b, i], where)

        def z_copy(i, src, dst, where):
            return remote(src, dst, z_send.at[b, i], z_recv.at[b, i], where)

        y_copies.append(
            [
                y_copy(0, piece.at[b, 2, :, :, one], y_far.at[b, :, :, one], up),
                y_copy(1, piece.at[b, 2, :, :, two], y_far.at[b, :, :, two], down),
                y_copy(2, piece.at[b, 1, :, :, two], y_left.at[b, :, :, two], up),
                y_copy(3, piece.at[b, 3, :, :, one], y_right.at[b, :, :, one], down),
                y_copy(4, piece.at[b, 1, :, :, one], y_left.at[b, :, :, one], up),
                y_copy(5, piece.at[b, 3, :, :, two], y_right.at[b, :, :, two], down),
            ]
        )
        z_copies.append(
            [
                z_copy(0, joined.at[b, 2, :, one], z_far.at[b, :, one], above),
                z_copy(1, joined.at[b, 2, :, two], z_far.at[b, :, two], under),
                z_copy(2, joined.at[b, 1, :, two], z_left.at[b, :, two], above),
                z_copy(3, joined.at[b, 3, :, one], z_right.at[b, :, one], under),
                z_copy(4, joined.at[b, 1, :, one], z_left.at[b, :, one], above),
                z_copy(5, joined.at[b, 3, :, two], z_right.at[b, :, two], under),
            ]
        )

    def associate(b):
        for copy in lon_copies[b]:
            copy.wait_recv()
        sign = (1 - 2 * hemisphere).astype(jnp.float32)
        kept = zonal[b, hemisphere, chunk_of(lon), :]
        for dx in range(1, n_lon):
            kept = kept + lon_in[b, 0, dx]
        other = lon_in[b, 1, 0]
        for dx in range(1, n_lon):
            other = other + lon_in[b, 1, dx]
        for parity, value in enumerate((kept + other, sign * (kept - other))):
            for part in range(2):
                block = value[part * slots : (part + 1) * slots]
                for i in range(PAIR):
                    cell = jnp.where(slot_lane < rows, turned(block, i * rows), 0.0)
                    top = cell.astype(jnp.bfloat16).astype(jnp.float32)
                    cell = top + turned(cell - top, -rows) + turned(top, -2 * rows)
                    left_side[pl.ds(parity * 8 + part * PAIR + i, slots, 16), :] = cell
        for dy in (2, 1, 3, 0):

            def one(dz, carry):
                slot = lax.rem(y + dy, RING) * RING + lax.rem(z + dz, RING)
                wave = waves[lon * slots + slot]
                left = left_side[pl.ds(pl.multiple_of(slot * 16, 16), 16), :].astype(jnp.bfloat16)
                product = jnp.dot(left, right_side[slot], preferred_element_type=jnp.float32)
                even = ((wave + column) & 1) == 0
                value = jnp.where(even, product[:8], product[8:])
                value = jnp.where(column >= wave, value, 0.0)
                piece[b, dy, dz] = jnp.where(row < 4, value[:, :half], pltpu.roll(value[:, half:], 4, 0))
                return carry

            for dz in range(RING):
                one(dz, 0)
            starts = {2: (0, 1), 1: (2,), 3: (3,), 0: ()}[dy]
            for i in starts:
                y_copies[b][i].start()

    def y_forward(b):
        one, two = big_of[b]
        y_copies[b][0].wait_recv()
        piece[b, 1, :, :, one] = piece[b, 1, :, :, one] + y_far[b, :, :, one]
        y_copies[b][4].start()
        y_copies[b][1].wait_recv()
        piece[b, 3, :, :, two] = piece[b, 3, :, :, two] + y_far[b, :, :, two]
        y_copies[b][5].start()

    def y_settle(b):
        for i in range(2, 6):
            y_copies[b][i].wait_recv()
        joined[b] = piece[b, 0] + y_left[b] + y_right[b]
        for i in range(4):
            z_copies[b][i].start()

    def z_forward(b):
        one, two = big_of[b]
        z_copies[b][0].wait_recv()
        joined[b, 1, :, one] = joined[b, 1, :, one] + z_far[b, :, one]
        z_copies[b][4].start()
        z_copies[b][1].wait_recv()
        joined[b, 3, :, two] = joined[b, 3, :, two] + z_far[b, :, two]
        z_copies[b][5].start()

    degree = lax.broadcasted_iota(jnp.int32, (8, half), 1) + jnp.where(row >= 4, half, 0)
    degree = degree.astype(jnp.float32)
    degree = degree * (degree + 1.0)

    def z_settle(b):
        damping = jnp.where(row % PAIR == 0, helm[PAIR * b], helm[PAIR * b + 1]) * degree + 1.0
        for i in range(2, 6):
            z_copies[b][i].wait_recv()
        result = (joined[b, 0] + z_left[b] + z_right[b]) / damping
        for r in range(8):
            h, part, i = r // 4, r // 2 % 2, r % 2
            at = part * degrees + h * half
            out[PAIR * b + i, 0, :, at : at + half] = result[r : r + 1]

    interior(0)
    send_rows(1)
    interior(1)
    corners()
    edges(0)
    transform(0)
    send_rows(2)
    interior(2)
    edges(1)
    transform(1)
    associate(0)
    edges(2)
    transform(2)
    associate(1)
    y_forward(0)
    associate(2)
    y_forward(1)
    y_settle(0)
    y_forward(2)
    y_settle(1)
    z_forward(0)
    y_settle(2)
    z_forward(1)
    z_forward(2)
    z_settle(0)
    z_settle(1)
    z_settle(2)
    for b in range(BATCHES):
        for copy in lon_copies[b] + y_copies[b] + z_copies[b]:
            copy.wait_send()


def spectrum_of(wave_map, helm, field, shifts, fracs, legendre):
    levels, rows, cols = field.shape
    n_lat, n_lon = lax.axis_size("lat"), lax.axis_size("lon")
    slots, _, degrees = legendre.shape
    vmem = pl.BlockSpec(memory_space=pltpu.VMEM)
    smem = pl.BlockSpec(memory_space=pltpu.SMEM)
    anywhere = pl.BlockSpec(memory_space=pl.ANY)
    halo_rows = levels * HALO
    side_tiles = pl.cdiv(levels * rows, LANES)
    f32 = jnp.float32
    full = 2 * wave_map.shape[0]
    chunk = full // n_lon
    count = cols // LANES
    block = (8, degrees // 2)
    dma = pltpu.SemaphoreType.DMA
    source = pltpu.VMEM((levels // 2, 2 * HALO, count, rows + 2 * HEAD, LANES), f32)
    return pl.pallas_call(
        functools.partial(fused_kernel, n_lat, n_lon),
        in_specs=[smem, smem, vmem] + [anywhere] * 5,
        out_specs=vmem,
        out_shape=jax.ShapeDtypeStruct((levels // 2, 1, 1, 2 * degrees), f32),
        scratch_shapes=[
            pltpu.VMEM((levels, rows, cols), jnp.int32),
            pltpu.VMEM((levels, rows, cols), jnp.int32),
            pltpu.VMEM((levels, rows, cols), jnp.bfloat16),
            pltpu.VMEM((levels, rows, cols), jnp.bfloat16),
            pltpu.VMEM((slots, rows, degrees), f32),
            pltpu.VMEM((2, halo_rows, cols), f32),
            pltpu.VMEM((2, 2, 8, LANES), f32),
            pltpu.VMEM((2, side_tiles, 8, LANES), f32),
            pltpu.VMEM((2, halo_rows, cols), f32),
            pltpu.VMEM((2, levels, rows, LANES), f32),
            pltpu.VMEM((2, side_tiles, 8, LANES), f32),
            pltpu.VMEM((2, 2, 8, LANES), f32),
            pltpu.VMEM((2, 2, halo_rows, LANES), f32),
            pltpu.VMEM((levels, rows, cols), f32),
            pltpu.VMEM((levels, rows, cols), f32),
            source,
            source,
            pltpu.VMEM((BATCHES, 2 * LANES, cols), f32),
            pltpu.VMEM((2 * full, cols), f32),
            pltpu.VMEM((BATCHES, 2, full, LANES), f32),
            pltpu.VMEM((BATCHES, 2, n_lon, chunk, LANES), f32),
            pltpu.VMEM((slots * 16, LANES), f32),
            pltpu.VMEM((slots, LANES, degrees), jnp.bfloat16),
            pltpu.VMEM((BATCHES, RING, RING) + block, f32),
            pltpu.VMEM((BATCHES, RING) + block, f32),
            pltpu.VMEM((BATCHES, RING) + block, f32),
            pltpu.VMEM((BATCHES, RING) + block, f32),
            pltpu.VMEM((BATCHES, RING) + block, f32),
            pltpu.VMEM((BATCHES,) + block, f32),
            pltpu.VMEM((BATCHES,) + block, f32),
            pltpu.VMEM((BATCHES,) + block, f32),
            dma((5,)),
            dma((2, BATCHES)),
            dma((2, BATCHES)),
            dma((2,)),
            dma((2,)),
            dma((2, 2)),
            dma((2, 2)),
            dma((BATCHES, 2, n_lon)),
            dma((BATCHES, 2, n_lon)),
            dma((BATCHES, 6)),
            dma((BATCHES, 6)),
            dma((BATCHES, 6)),
            dma((BATCHES, 6)),
        ],
        compiler_params=pltpu.CompilerParams(
            collective_id=0, has_side_effects=True, vmem_limit_bytes=VMEM_BYTES
        ),
        name="spectrum",
    )(wave_map, helm, field, *shifts, *fracs, legendre)


def local(field, row_shift, col_shift, row_frac, col_frac, wave_map, legendre, helm_coef):
    return spectrum_of(
        wave_map,
        helm_coef,
        field[0],
        (row_shift[0], col_shift[0]),
        (row_frac[0], col_frac[0]),
        legendre,
    )


def solution(mesh):
    block = P("fold", None, "lat", "lon")
    in_specs = (block,) * 5 + (P(), P("lon", "lat", None), P("fold"))
    out_specs = P("fold", "lon", "lat", None)
    return jax.shard_map(local, mesh=mesh, in_specs=in_specs, out_specs=out_specs, check_vma=False)
```
